32 devices in a mesh: grp: 2 (over y), seq: 8 (over z, x), tp: 2 (over core).
Axes of the slice: x: 2, y: 2, z: 4, core: 2. Of those that a mesh axis runs over, the one named last changes fastest.
Arguments:
- hidden: bfloat16 [8, 8192], P('grp', 'seq'), parts along dimension 0, may hold values from -40 to 40
- norm_gain: float32 [8192], P('seq'), may hold values from 0.25 to 1.75
- query_proj: bfloat16 [8192, 4096], P('seq', 'tp'), may hold values from -0.0625 to 0.0625
- keyval_proj: bfloat16 [8192, 2, 512], P('seq', None, 'tp'), may hold values from -0.0625 to 0.0625
- attend_proj: bfloat16 [4096, 8192], P('tp', 'seq'), may hold values from -0.09375 to 0.09375
- keyval_cache: bfloat16 [2, 8, 512, 512], P(None, 'grp', 'seq', 'tp'), parts along dimension 1, may hold values from -320 to 320
- lengths: int32 [8], P('grp'), parts along dimension 0, may hold values from 1 to 512, as said below
Outputs:
- hidden_out: bfloat16 [8, 8192], P('grp', 'seq'), parts along dimension 0
- new_keyval: bfloat16 [8, 2, 512], P('grp', None, 'tp'), parts along dimension 0
The draws below stay inside these ranges and needn't reach their ends.
There are 2 independent parts, one for each index of `grp`. The reference program is written for one: setup_inputs(seed, part) draws one part's arguments, and reference() takes and returns one part's arrays. A program takes and returns all parts, laid end to end along the dimension named above; an argument that names none is the same for every part. Nothing has to cross between parts.
Inputs may be any that keep to these rules, and one draw needn't show every extreme that they name: `lengths`: live cached positions of each request; in every draw some request has all 512.
All inputs are finite; a program needn't handle non-finite values.
Results may differ from the reference program's by a relative error of at most 0.0087.
Values sent between devices are 32-bit elements; how exact they have to be, the bound alone decides.
A program may use at most 64 MiB of HBM per device.

```python
import jax
import jax.numpy as jnp
from jax import lax

D = 8192
QHEADS = 32
KVHEADS = 4
HEAD_DIM = 128
ROWS = 4
CTX_DEV = 64
CTX = 512
N_SEQ = 8


def draw_hidden(key, part):
    noise_key, row_key = jax.random.split(jax.random.fold_in(key, 11), 2)
    columns = jnp.arange(D, dtype=jnp.float32) / D
    row_factor = 10.0 ** jax.random.uniform(row_key, (ROWS, 1), jnp.float32, -0.5, 0.5)
    noise = jnp.clip(jax.random.normal(noise_key, (ROWS, D), jnp.float32), -4.0, 4.0)
    column_factor = 10.0 ** (0.5 * columns - 0.25)
    return jnp.clip(noise * row_factor * column_factor[None, :], -40.0, 40.0).astype(jnp.bfloat16)


def draw_keyval_cache(key, part):
    noise_key = jax.random.fold_in(jax.random.fold_in(key, 23), 0)
    noise = jnp.clip(jax.random.normal(noise_key, (2, ROWS, CTX, KVHEADS * HEAD_DIM), jnp.float32), -5.0, 5.0)
    return jnp.clip(noise, -320.0, 320.0).astype(jnp.bfloat16)


def draw_lengths(key, part):
    length_key, row_key = jax.random.split(jax.random.fold_in(key, 37))
    drawn = jax.random.randint(length_key, (ROWS,), 1, CTX + 1)
    longest = jax.random.randint(row_key, (), 0, ROWS)
    return jnp.where(jnp.arange(ROWS) == longest, CTX, drawn).astype(jnp.int32)


def levels(stream_key, shape, cuts, least, high):
    level, own = 1.0, jax.random.fold_in(stream_key, 6)
    for position, blocks in cuts:
        steps = jnp.exp(jax.random.uniform(jax.random.fold_in(own, position), (blocks,), jnp.float32, least / len(cuts), high / len(cuts)))
        level = level * jnp.repeat(steps, shape[position] // blocks).reshape([-1 if axis == position else 1 for axis in range(len(shape))])
    return level


def gaussian(rng, dims, scale, limit, shards=(), held_as=jnp.bfloat16):
    values = jax.random.normal(rng, dims, jnp.float32) * scale
    if len(shards) > 0:
        values = levels(rng, dims, shards, -0.22, 0.18) * values
    return jnp.clip(values, min=-limit, max=limit).astype(held_as)


def setup_inputs(seed: int = 0, part: int = 0) -> dict:
    key_list = jax.random.split(jax.random.key(seed), 8)
    part_splits = jax.random.split(jax.random.fold_in(key_list[7], part), 8)
    return {
        "hidden": draw_hidden(jax.random.fold_in(jax.random.fold_in(key_list[7], part), 71), part),
        "norm_gain": jnp.clip(1.0 + 0.15 * jax.random.normal(key_list[1], (D,), jnp.float32), 0.25, 1.75),
        "query_proj": gaussian(key_list[2], (D, QHEADS * HEAD_DIM), D ** -0.5, 0.0625, ((0, 8), (1, 2))),
        "keyval_proj": gaussian(key_list[3], (D, 2, KVHEADS * HEAD_DIM), D ** -0.5, 0.0625, ((0, 8), (2, 2))),
        "attend_proj": gaussian(key_list[4], (QHEADS * HEAD_DIM, D), (QHEADS * HEAD_DIM) ** -0.5, 0.09375, ((0, 2), (1, 8))),
        "keyval_cache": draw_keyval_cache(jax.random.fold_in(jax.random.fold_in(key_list[7], part), 71), part),
        "lengths": draw_lengths(jax.random.fold_in(jax.random.fold_in(key_list[7], part), 71), part),
    }


EPSILON = 1e-05
MASKED = -1e+30

def reference(hidden, norm_gain, query_proj, keyval_proj, attend_proj, keyval_cache, lengths):
    row_count = hidden.shape[0]
    one_float = hidden.astype(jnp.float32)
    scale_two = lax.rsqrt(lax.optimization_barrier(jnp.mean(one_float * one_float, axis=1)) + EPSILON)[:, None]
    scaled = (one_float * norm_gain).astype(jnp.bfloat16)
    query = (jnp.dot(scaled, query_proj, preferred_element_type=jnp.float32) * scale_two).astype(jnp.bfloat16)
    new_keyval = (jnp.dot(scaled, keyval_proj.reshape(D, 2 * KVHEADS * HEAD_DIM), preferred_element_type=jnp.float32).reshape(row_count, 2, KVHEADS * HEAD_DIM) * scale_two[:, :, None]).astype(jnp.bfloat16)
    group_share = QHEADS // KVHEADS
    score_scale = HEAD_DIM ** (-0.5)
    query_heads = query.reshape(row_count, KVHEADS, group_share, HEAD_DIM).astype(jnp.float32)
    cache_keys = keyval_cache[0].reshape(row_count, N_SEQ, CTX_DEV, KVHEADS, HEAD_DIM).astype(jnp.float32)
    cache_values = keyval_cache[1].reshape(row_count, N_SEQ, CTX_DEV, KVHEADS, HEAD_DIM).astype(jnp.float32)
    scores = jnp.einsum('rkgd,rbskd->rbkgs', query_heads, cache_keys, precision=lax.Precision.HIGHEST) * score_scale
    positions = jnp.arange(CTX, dtype=jnp.int32).reshape(N_SEQ, CTX_DEV)
    live_mask = (positions[None] < lengths[:, None, None])[:, :, None, None, :]
    scores = jnp.where(live_mask, scores, MASKED)
    block_max = lax.optimization_barrier(jnp.max(scores, axis=4))
    weights = jnp.where(live_mask, jnp.exp(scores - block_max[..., None]), 0.0).astype(jnp.bfloat16)
    weights = lax.optimization_barrier(weights).astype(jnp.float32)
    block_total = lax.optimization_barrier(jnp.sum(weights, axis=4))
    block_out = jnp.einsum('rbkgs,rbskd->rbkgd', weights, cache_values, precision=lax.Precision.HIGHEST)
    best_score = lax.optimization_barrier(jnp.max(block_max, axis=1))
    factor = jnp.exp(block_max - best_score[:, None])
    total_weight = lax.optimization_barrier(jnp.sum(factor * block_total, axis=1))
    gathered = lax.optimization_barrier(jnp.sum(factor[..., None] * block_out, axis=1))
    own_key = new_keyval[:, 0].reshape(row_count, KVHEADS, HEAD_DIM).astype(jnp.float32)
    own_value = new_keyval[:, 1].reshape(row_count, KVHEADS, HEAD_DIM).astype(jnp.float32)
    own_score = jnp.einsum('rkgd,rkd->rkg', query_heads, own_key, precision=lax.Precision.HIGHEST) * score_scale
    top_score = jnp.maximum(best_score, own_score)
    old_weight = jnp.exp(best_score - top_score)
    fresh_weight = jnp.exp(own_score - top_score)
    attended = (old_weight[..., None] * gathered + fresh_weight[..., None] * own_value[:, :, None, :]) / (old_weight * total_weight + fresh_weight)[..., None]
    attended = attended.reshape(row_count, QHEADS * HEAD_DIM).astype(jnp.bfloat16)
    hidden_out = (one_float + jnp.dot(attended, attend_proj, preferred_element_type=jnp.float32)).astype(jnp.bfloat16)
    return (hidden_out, new_keyval)
```

```python
import functools

import jax
import jax.numpy as jnp
from jax import lax
from jax.experimental import pallas as pl
from jax.experimental.pallas import tpu as pltpu
from jax.sharding import PartitionSpec as P

D = 8192
HEAD_DIM = 128


EPSILON = 1e-05
MASKED = -1e30


def on_device(hidden, norm_gain, query_proj, keyval_proj, attend_proj, keyval_cache, lengths):
    row_count = hidden.shape[0]
    feature_dev = hidden.shape[1]
    seq_rank = lax.axis_index("seq")
    ctx_dev = keyval_cache.shape[2]
    kv_width = keyval_cache.shape[3]
    kv_heads = kv_width // HEAD_DIM
    q_heads = query_proj.shape[1] // HEAD_DIM
    group_share = q_heads // kv_heads
    score_scale = HEAD_DIM ** (-0.5)
    one_float = hidden.astype(jnp.float32)
    scaled = (one_float * norm_gain).astype(jnp.bfloat16)
    squares = jnp.sum(one_float * one_float, axis=1)
    query_part = jnp.dot(scaled, query_proj, preferred_element_type=jnp.float32)
    keyval_part = jnp.dot(
        scaled, keyval_proj.reshape(feature_dev, 2 * kv_width), preferred_element_type=jnp.float32
    ).reshape(row_count, 2, kv_width)
    query_sum, keyval_sum, squares_sum = lax.psum((query_part, keyval_part, squares), "seq")
    scale_two = lax.rsqrt(squares_sum / D + EPSILON)[:, None]
    query = (query_sum * scale_two).astype(jnp.bfloat16)
    new_keyval = (keyval_sum * scale_two[:, :, None]).astype(jnp.bfloat16)
    query_heads = query.reshape(row_count, kv_heads, group_share, HEAD_DIM)
    cache_keys = keyval_cache[0].reshape(row_count, ctx_dev, kv_heads, HEAD_DIM)
    cache_values = keyval_cache[1].reshape(row_count, ctx_dev, kv_heads, HEAD_DIM)
    scores = (
        jnp.einsum("rkgd,rskd->rkgs", query_heads, cache_keys, preferred_element_type=jnp.float32)
        * score_scale
    )
    positions = seq_rank * ctx_dev + jnp.arange(ctx_dev, dtype=jnp.int32)
    live_mask = (positions[None, :] < lengths[:, None])[:, None, None, :]
    scores = jnp.where(live_mask, scores, MASKED)
    block_max = jnp.max(scores, axis=3)
    weights = jnp.where(live_mask, jnp.exp(scores - block_max[..., None]), 0.0).astype(jnp.bfloat16)
    block_total = jnp.sum(lax.optimization_barrier(weights).astype(jnp.float32), axis=3)
    block_out = jnp.einsum(
        "rkgs,rskd->rkgd", weights, cache_values, preferred_element_type=jnp.float32
    )
    best_score = lax.pmax(block_max, "seq")
    factor = jnp.exp(block_max - best_score)
    total_weight, gathered = lax.psum((block_total * factor, block_out * factor[..., None]), "seq")
    own_key = new_keyval[:, 0].reshape(row_count, kv_heads, HEAD_DIM)
    own_value = new_keyval[:, 1].reshape(row_count, kv_heads, HEAD_DIM).astype(jnp.float32)
    own_score = (
        jnp.einsum("rkgd,rkd->rkg", query_heads, own_key, preferred_element_type=jnp.float32)
        * score_scale
    )
    top_score = jnp.maximum(best_score, own_score)
    old_weight = jnp.exp(best_score - top_score)
    fresh_weight = jnp.exp(own_score - top_score)
    attended = (
        old_weight[..., None] * gathered + fresh_weight[..., None] * own_value[:, :, None, :]
    ) / (old_weight * total_weight + fresh_weight)[..., None]
    attended = attended.reshape(row_count, q_heads * HEAD_DIM).astype(jnp.bfloat16)
    attend_term = jnp.dot(attended, attend_proj, preferred_element_type=jnp.float32)
    hidden_out = (one_float + lax.psum(attend_term, "tp")).astype(jnp.bfloat16)
    return (hidden_out, new_keyval)


MESH = pl.DeviceIdType.MESH
F32 = jnp.float32
BF16 = jnp.bfloat16
QUERY_PIECES = 4
OUT_PIECES = 4


def fused_kernel(
    n,
    hidden_ref,
    gain_ref,
    lengths_ref,
    query_hbm,
    keyval_hbm,
    attend_hbm,
    cache_hbm,
    out_ref,
    kv_out_ref,
    query_w,
    keyval_w,
    attend_w,
    cache,
    sums_out,
    sums_in,
    sums_mine,
    sums_all,
    soft_out,
    soft_in,
    att_mine,
    att_all,
    term_mine,
    term_in,
    load_sem,
    send_sem,
    recv_sem,
):
    me = lax.axis_index("seq")
    core = lax.axis_index("tp")
    rows, feature_dev = hidden_ref.shape
    width = query_w.shape[1]
    q_heads = width // HEAD_DIM
    ctx_dev = cache.shape[2]
    kv_heads = cache.shape[3] // HEAD_DIM
    share = q_heads // kv_heads
    per = q_heads // n
    block = per * rows
    kv_rows = 2 * kv_heads * rows
    kv_per = kv_rows // n
    score_scale = HEAD_DIM ** (-0.5)

    step = width // QUERY_PIECES
    kv_load = pltpu.make_async_copy(keyval_hbm, keyval_w, load_sem.at[0])
    kv_load.start()
    query_loads = []
    for piece in range(QUERY_PIECES):
        cols = pl.ds(piece * step, step)
        load = pltpu.make_async_copy(
            query_hbm.at[:, cols], query_w.at[:, cols], load_sem.at[1 + piece]
        )
        load.start()
        query_loads.append(load)
    cache_load = pltpu.make_async_copy(cache_hbm, cache, load_sem.at[1 + QUERY_PIECES])
    cache_load.start()
    out_loads = []
    depth = width // OUT_PIECES
    for piece in range(OUT_PIECES):
        part = pl.ds(piece * depth, depth)
        load = pltpu.make_async_copy(
            attend_hbm.at[part], attend_w.at[part], load_sem.at[2 + QUERY_PIECES + piece]
        )
        load.start()
        out_loads.append(load)

    barrier = pltpu.get_barrier_semaphore()
    for k in range(1, n):
        pl.semaphore_signal(
            barrier, inc=1, device_id={"seq": lax.rem(me + k, n)}, device_id_type=MESH
        )
    pl.semaphore_signal(barrier, inc=1, device_id={"tp": 1 - core}, device_id_type=MESH)

    one_float = hidden_ref[...].astype(F32)
    scaled = one_float * gain_ref[...]
    scaled_b = scaled.astype(BF16)
    squares = jnp.sum(one_float * one_float, axis=1, keepdims=True)
    squares = jnp.broadcast_to(squares, (rows, HEAD_DIM))

    parts = 2 * kv_heads
    groups = feature_dev // HEAD_DIM
    span = HEAD_DIM * parts
    stacked = jnp.concatenate(
        [scaled[:, g * HEAD_DIM : (g + 1) * HEAD_DIM] for g in range(groups)], axis=0
    ).astype(BF16)
    spread_row = lax.broadcasted_iota(jnp.int32, (HEAD_DIM, span), 0)
    spread_col = lax.broadcasted_iota(jnp.int32, (HEAD_DIM, span), 1)
    spread = jnp.where(spread_col // parts == spread_row, 1.0, 0.0).astype(BF16)
    wide = jnp.dot(stacked, spread, preferred_element_type=F32)
    pick_row = lax.broadcasted_iota(jnp.int32, (kv_rows, span), 0) // rows
    pick_col = lax.broadcasted_iota(jnp.int32, (kv_rows, span), 1) % parts
    pick = pick_row == pick_col
    left = jnp.concatenate(
        [
            jnp.where(
                pick, jnp.concatenate([wide[g * rows : (g + 1) * rows]] * parts, axis=0), 0.0
            ).astype(BF16)
            for g in range(groups)
        ],
        axis=1,
    )
    kv_load.wait()
    keyval_part = jnp.dot(left, keyval_w[...], preferred_element_type=F32)
    for c in range(n):
        sums_out[c, block : block + kv_per, :] = keyval_part[c * kv_per : (c + 1) * kv_per]
        sums_out[c, block + kv_per : block + kv_per + rows, :] = squares

    for piece in range(QUERY_PIECES):
        query_loads[piece].wait()
        product = jnp.dot(
            scaled_b, query_w[:, piece * step : (piece + 1) * step], preferred_element_type=F32
        )
        for h in range(step // HEAD_DIM):
            head = piece * (step // HEAD_DIM) + h
            low = (head % per) * rows
            sums_out[head // per, low : low + rows, :] = product[
                :, h * HEAD_DIM : (h + 1) * HEAD_DIM
            ]

    pl.semaphore_wait(barrier, n)

    pending = []

    def send(source, target, phase, k):
        copy = pltpu.make_async_remote_copy(
            src_ref=source,
            dst_ref=target,
            send_sem=send_sem.at[phase, k],
            recv_sem=recv_sem.at[phase, k],
            device_id={"seq": lax.rem(me + k, n)},
            device_id_type=MESH,
        )
        copy.start()
        pending.append(copy)
        return copy

    copies = [
        send(sums_out.at[lax.rem(me + k, n)], sums_in.at[k], 0, k) for k in range(1, n)
    ]
    total = sums_out[me]
    for k in range(1, n):
        copies[k - 1].wait_recv()
        total = total + sums_in[k]
    sums_mine[...] = total

    copies = [send(sums_mine, sums_all.at[me], 1, k) for k in range(1, n)]
    sums_all[me] = total

    cols = rows * ctx_dev
    mask_row = lax.broadcasted_iota(jnp.int32, (share * rows, cols), 0) % rows
    mask_col = lax.broadcasted_iota(jnp.int32, (share * rows, cols), 1)
    limit = jnp.zeros((share * rows, cols), jnp.int32)
    for r in range(rows):
        limit = jnp.where(mask_col // ctx_dev == r, lengths_ref[r], limit)
    position = me * ctx_dev + mask_col % ctx_dev
    live = jnp.logical_and(mask_row == mask_col // ctx_dev, position < limit)
    cache_load.wait()

    for copy in copies:
        copy.wait_recv()
    squares_sum = sums_all[0, block + kv_per : block + kv_per + rows, :]
    scale = lax.rsqrt(squares_sum / (feature_dev * n) + EPSILON)
    scale_block = jnp.concatenate([scale] * per, axis=0)
    chunk_heads = share // per
    lane = lax.broadcasted_iota(jnp.int32, (share * rows, HEAD_DIM), 1)
    for head in range(kv_heads):
        query = jnp.concatenate(
            [
                sums_all[c, :block, :] * scale_block
                for c in range(head * chunk_heads, (head + 1) * chunk_heads)
            ],
            axis=0,
        ).astype(BF16)
        lanes = slice(head * HEAD_DIM, (head + 1) * HEAD_DIM)
        keys = cache[0, :, :, lanes].reshape(cols, HEAD_DIM)
        values = cache[1, :, :, lanes].reshape(cols, HEAD_DIM)
        scores = (
            lax.dot_general(
                query, keys, (((1,), (1,)), ((), ())), preferred_element_type=F32
            )
            * score_scale
        )
        scores = jnp.where(live, scores, MASKED)
        block_max = jnp.max(scores, axis=1, keepdims=True)
        weights = jnp.where(live, jnp.exp(scores - block_max), 0.0).astype(BF16)
        block_total = jnp.sum(weights.astype(F32), axis=1, keepdims=True)
        block_out = jnp.dot(weights, values, preferred_element_type=F32)
        stats = jnp.where(lane < HEAD_DIM // 2, block_max, block_total)
        for c in range(chunk_heads):
            part = slice(c * block, (c + 1) * block)
            soft_out[head * chunk_heads + c, :block, :] = block_out[part]
            soft_out[head * chunk_heads + c, block : 2 * block, :] = stats[part]

    copies = [
        send(soft_out.at[lax.rem(me + k, n)], soft_in.at[k], 2, k) for k in range(1, n)
    ]

    keyval = jnp.concatenate(
        [sums_all[c, block : block + kv_per, :] for c in range(n)], axis=0
    )
    keyval = (keyval * jnp.concatenate([scale] * parts, axis=0)).astype(BF16).astype(F32)
    kv_out_ref[...] = keyval
    mine = me // chunk_heads
    own_key = keyval[:rows]
    own_value = keyval[rows : 2 * rows]
    for head in range(1, kv_heads):
        here = mine == head
        own_key = jnp.where(here, keyval[2 * head * rows : (2 * head + 1) * rows], own_key)
        own_value = jnp.where(
            here, keyval[(2 * head + 1) * rows : (2 * head + 2) * rows], own_value
        )
    own_key = jnp.concatenate([own_key] * per, axis=0)
    own_value = jnp.concatenate([own_value] * per, axis=0)
    query = (sums_all[me, :block, :] * scale_block).astype(BF16).astype(F32)
    own_score = jnp.sum(query * own_key, axis=1, keepdims=True) * score_scale

    for copy in copies:
        copy.wait_recv()
    chunks = [(soft_out[me, :block, :], soft_out[me, block : 2 * block, :])]
    chunks += [(soft_in[k, :block, :], soft_in[k, block : 2 * block, :]) for k in range(1, n)]
    maxes = [stats[:, :1] for _, stats in chunks]
    totals = [stats[:, HEAD_DIM // 2 : HEAD_DIM // 2 + 1] for _, stats in chunks]
    best = functools.reduce(jnp.maximum, maxes)
    top = jnp.maximum(best, own_score)
    fresh = jnp.exp(own_score - top)
    over = fresh * own_value
    under = fresh
    for (values, _), block_max, block_total in zip(chunks, maxes, totals):
        factor = jnp.exp(block_max - top)
        over = over + factor * values
        under = under + factor * block_total
    attended = (over / under).astype(BF16).astype(F32)
    att_mine[...] = attended

    copies = [send(att_mine, att_all.at[me], 3, k) for k in range(1, n)]
    att_all[me] = attended
    for load in out_loads:
        load.wait()
    for copy in copies:
        copy.wait_recv()
    attended = jnp.concatenate(
        [
            att_all[head // per, (head % per) * rows : (head % per + 1) * rows, :]
            for head in range(q_heads)
        ],
        axis=1,
    ).astype(BF16)
    term = jnp.dot(attended, attend_w[...], preferred_element_type=F32)
    term_mine[...] = term
    swap = pltpu.make_async_remote_copy(
        src_ref=term_mine,
        dst_ref=term_in,
        send_sem=send_sem.at[0, 0],
        recv_sem=recv_sem.at[0, 0],
        device_id={"tp": 1 - core},
        device_id_type=MESH,
    )
    swap.start()
    for copy in pending:
        copy.wait_send()
    swap.wait()
    out_ref[...] = (one_float + (term + term_in[...])).astype(out_ref.dtype)


def fused_device(n, hidden, norm_gain, query_proj, keyval_proj, attend_proj, keyval_cache, lengths):
    rows, feature_dev = hidden.shape
    width = query_proj.shape[1]
    kv_width = keyval_proj.shape[2]
    kv_heads = kv_width // HEAD_DIM
    block = width // HEAD_DIM // n * rows
    kv_rows = 2 * kv_heads * rows
    chunk = -(-(block + kv_rows // n + rows) // 8) * 8
    out_width = attend_proj.shape[1]
    stored = keyval_proj.reshape(feature_dev, 2, kv_heads, HEAD_DIM).transpose(0, 2, 1, 3)
    stored = stored.reshape(feature_dev * 2 * kv_heads, HEAD_DIM)
    vmem = pl.BlockSpec(memory_space=pltpu.VMEM)
    hbm = pl.BlockSpec(memory_space=pl.ANY)
    hidden_out, keyval = pl.pallas_call(
        functools.partial(fused_kernel, n),
        out_shape=(
            jax.ShapeDtypeStruct((rows, out_width), BF16),
            jax.ShapeDtypeStruct((kv_rows, HEAD_DIM), F32),
        ),
        in_specs=[vmem, vmem, pl.BlockSpec(memory_space=pltpu.SMEM), hbm, hbm, hbm, hbm],
        out_specs=(vmem, vmem),
        scratch_shapes=[
            pltpu.VMEM(query_proj.shape, BF16),
            pltpu.VMEM(stored.shape, BF16),
            pltpu.VMEM(attend_proj.shape, BF16),
            pltpu.VMEM(keyval_cache.shape, BF16),
            pltpu.VMEM((n, chunk, HEAD_DIM), F32),
            pltpu.VMEM((n, chunk, HEAD_DIM), F32),
            pltpu.VMEM((chunk, HEAD_DIM), F32),
            pltpu.VMEM((n, chunk, HEAD_DIM), F32),
            pltpu.VMEM((n, 2 * block, HEAD_DIM), F32),
            pltpu.VMEM((n, 2 * block, HEAD_DIM), F32),
            pltpu.VMEM((block, HEAD_DIM), F32),
            pltpu.VMEM((n, block, HEAD_DIM), F32),
            pltpu.VMEM((rows, out_width), F32),
            pltpu.VMEM((rows, out_width), F32),
            pltpu.SemaphoreType.DMA((2 + QUERY_PIECES + OUT_PIECES,)),
            pltpu.SemaphoreType.DMA((4, n)),
            pltpu.SemaphoreType.DMA((4, n)),
        ],
        compiler_params=pltpu.CompilerParams(collective_id=0, has_side_effects=True),
    )(
        hidden,
        norm_gain.reshape(1, feature_dev),
        lengths,
        query_proj,
        stored,
        attend_proj,
        keyval_cache,
    )
    new_keyval = keyval.reshape(kv_heads, 2, rows, HEAD_DIM).transpose(2, 1, 0, 3)
    return hidden_out, new_keyval.reshape(rows, 2, kv_width).astype(BF16)


def fits(n, cores, hidden, norm_gain, query_proj, keyval_proj, attend_proj, keyval_cache, lengths):
    rows, feature_dev = hidden.shape
    q_heads = query_proj.shape[1] // HEAD_DIM
    kv_heads = keyval_proj.shape[2] // HEAD_DIM
    if q_heads % n or (2 * kv_heads * rows) % n or cores != 2 or n < 2:
        return False
    per = q_heads // n
    return (
        (q_heads // kv_heads) % per == 0
        and (per * rows) % 8 == 0
        and feature_dev % HEAD_DIM == 0
        and keyval_cache.shape[2] % 16 == 0
        and query_proj.shape[1] % (HEAD_DIM * QUERY_PIECES) == 0
    )


def pick_device(n, cores, *arrays):
    if fits(n, cores, *arrays):
        return fused_device(n, *arrays)
    return on_device(*arrays)


def solution(mesh):
    in_specs = (
        P("grp", "seq"),
        P("seq"),
        P("seq", "tp"),
        P("seq", None, "tp"),
        P("tp", "seq"),
        P(None, "grp", "seq", "tp"),
        P("grp"),
    )
    out_specs = (P("grp", "seq"), P("grp", None, "tp"))
    body = functools.partial(pick_device, mesh.shape["seq"], mesh.shape["tp"])
    return jax.shard_map(
        body, mesh=mesh, in_specs=in_specs, out_specs=out_specs, check_vma=False
    )
```

```python
import functools

import jax
import jax.numpy as jnp
from jax import lax
from jax.experimental import pallas as pl
from jax.experimental.pallas import tpu as pltpu
from jax.sharding import PartitionSpec as P

D = 8192
HEAD_DIM = 128


EPSILON = 1e-05
MASKED = -1e30


def on_device(hidden, norm_gain, query_proj, keyval_proj, attend_proj, keyval_cache, lengths):
    row_count = hidden.shape[0]
    feature_dev = hidden.shape[1]
    seq_rank = lax.axis_index("seq")
    ctx_dev = keyval_cache.shape[2]
    kv_width = keyval_cache.shape[3]
    kv_heads = kv_width // HEAD_DIM
    q_heads = query_proj.shape[1] // HEAD_DIM
    group_share = q_heads // kv_heads
    score_scale = HEAD_DIM ** (-0.5)
    one_float = hidden.astype(jnp.float32)
    scaled = (one_float * norm_gain).astype(jnp.bfloat16)
    squares = jnp.sum(one_float * one_float, axis=1)
    query_part = jnp.dot(scaled, query_proj, preferred_element_type=jnp.float32)
    keyval_part = jnp.dot(
        scaled, keyval_proj.reshape(feature_dev, 2 * kv_width), preferred_element_type=jnp.float32
    ).reshape(row_count, 2, kv_width)
    query_sum, keyval_sum, squares_sum = lax.psum((query_part, keyval_part, squares), "seq")
    scale_two = lax.rsqrt(squares_sum / D + EPSILON)[:, None]
    query = (query_sum * scale_two).astype(jnp.bfloat16)
    new_keyval = (keyval_sum * scale_two[:, :, None]).astype(jnp.bfloat16)
    query_heads = query.reshape(row_count, kv_heads, group_share, HEAD_DIM)
    cache_keys = keyval_cache[0].reshape(row_count, ctx_dev, kv_heads, HEAD_DIM)
    cache_values = keyval_cache[1].reshape(row_count, ctx_dev, kv_heads, HEAD_DIM)
    scores = (
        jnp.einsum("rkgd,rskd->rkgs", query_heads, cache_keys, preferred_element_type=jnp.float32)
        * score_scale
    )
    positions = seq_rank * ctx_dev + jnp.arange(ctx_dev, dtype=jnp.int32)
    live_mask = (positions[None, :] < lengths[:, None])[:, None, None, :]
    scores = jnp.where(live_mask, scores, MASKED)
    block_max = jnp.max(scores, axis=3)
    weights = jnp.where(live_mask, jnp.exp(scores - block_max[..., None]), 0.0).astype(jnp.bfloat16)
    block_total = jnp.sum(lax.optimization_barrier(weights).astype(jnp.float32), axis=3)
    block_out = jnp.einsum(
        "rkgs,rskd->rkgd", weights, cache_values, preferred_element_type=jnp.float32
    )
    best_score = lax.pmax(block_max, "seq")
    factor = jnp.exp(block_max - best_score)
    total_weight, gathered = lax.psum((block_total * factor, block_out * factor[..., None]), "seq")
    own_key = new_keyval[:, 0].reshape(row_count, kv_heads, HEAD_DIM)
    own_value = new_keyval[:, 1].reshape(row_count, kv_heads, HEAD_DIM).astype(jnp.float32)
    own_score = (
        jnp.einsum("rkgd,rkd->rkg", query_heads, own_key, preferred_element_type=jnp.float32)
        * score_scale
    )
    top_score = jnp.maximum(best_score, own_score)
    old_weight = jnp.exp(best_score - top_score)
    fresh_weight = jnp.exp(own_score - top_score)
    attended = (
        old_weight[..., None] * gathered + fresh_weight[..., None] * own_value[:, :, None, :]
    ) / (old_weight * total_weight + fresh_weight)[..., None]
    attended = attended.reshape(row_count, q_heads * HEAD_DIM).astype(jnp.bfloat16)
    attend_term = jnp.dot(attended, attend_proj, preferred_element_type=jnp.float32)
    hidden_out = (one_float + lax.psum(attend_term, "tp")).astype(jnp.bfloat16)
    return (hidden_out, new_keyval)


MESH = pl.DeviceIdType.MESH
F32 = jnp.float32
BF16 = jnp.bfloat16
QUERY_PIECES = 4
OUT_PIECES = 4


def fused_kernel(
    n,
    hidden_hbm,
    gain_hbm,
    lengths_hbm,
    query_hbm,
    keyval_hbm,
    attend_hbm,
    cache_hbm,
    out_ref,
    kv_out_ref,
    hidden_ref,
    gain_ref,
    lengths_ref,
    query_w,
    keyval_w,
    attend_w,
    cache,
    sums_out,
    sums_in,
    sums_mine,
    sums_all,
    soft_out,
    soft_in,
    att_mine,
    att_all,
    term_mine,
    term_in,
    load_sem,
    send_sem,
    recv_sem,
):
    me = lax.axis_index("seq")
    core = lax.axis_index("tp")
    rows, feature_dev = hidden_ref.shape
    width = query_w.shape[1]
    q_heads = width // HEAD_DIM
    ctx_dev = cache.shape[2]
    kv_heads = cache.shape[3] // HEAD_DIM
    share = q_heads // kv_heads
    per = q_heads // n
    block = per * rows
    kv_rows = 2 * kv_heads * rows
    kv_per = kv_rows // n
    score_scale = HEAD_DIM ** (-0.5)

    step = width // QUERY_PIECES
    barrier = pltpu.get_barrier_semaphore()
    for k in range(1, n):
        pl.semaphore_signal(
            barrier, inc=1, device_id={"seq": lax.rem(me + k, n)}, device_id_type=MESH
        )
    pl.semaphore_signal(barrier, inc=1, device_id={"tp": 1 - core}, device_id_type=MESH)

    small_loads = [
        pltpu.make_async_copy(source, target, load_sem.at[2 + QUERY_PIECES + OUT_PIECES + i])
        for i, (source, target) in enumerate(
            [(hidden_hbm, hidden_ref), (gain_hbm, gain_ref), (lengths_hbm, lengths_ref)]
        )
    ]
    for load in small_loads:
        load.start()
    kv_load = pltpu.make_async_copy(keyval_hbm, keyval_w, load_sem.at[0])
    kv_load.start()
    query_loads = []
    for piece in range(QUERY_PIECES):
        cols = pl.ds(piece * step, step)
        load = pltpu.make_async_copy(
            query_hbm.at[:, cols], query_w.at[:, cols], load_sem.at[1 + piece]
        )
        load.start()
        query_loads.append(load)
    for load in small_loads:
        load.wait()
    one_float = hidden_ref[...].astype(F32)
    scaled = one_float * gain_ref[...]
    scaled_b = scaled.astype(BF16)
    squares = jnp.sum(one_float * one_float, axis=1, keepdims=True)
    squares = jnp.broadcast_to(squares, (rows, HEAD_DIM))

    parts = 2 * kv_heads
    groups = feature_dev // HEAD_DIM
    span = HEAD_DIM * parts
    stacked = jnp.concatenate(
        [scaled[:, g * HEAD_DIM : (g + 1) * HEAD_DIM] for g in range(groups)], axis=0
    ).astype(BF16)
    spread_row = lax.broadcasted_iota(jnp.int32, (HEAD_DIM, span), 0)
    spread_col = lax.broadcasted_iota(jnp.int32, (HEAD_DIM, span), 1)
    spread = jnp.where(spread_col // parts == spread_row, 1.0, 0.0).astype(BF16)
    wide = jnp.dot(stacked, spread, preferred_element_type=F32)
    pick_row = lax.broadcasted_iota(jnp.int32, (kv_rows, span), 0) // rows
    pick_col = lax.broadcasted_iota(jnp.int32, (kv_rows, span), 1) % parts
    pick = pick_row == pick_col
    left = jnp.concatenate(
        [
            jnp.where(
                pick, jnp.concatenate([wide[g * rows : (g + 1) * rows]] * parts, axis=0), 0.0
            ).astype(BF16)
            for g in range(groups)
        ],
        axis=1,
    )
    kv_load.wait()
    keyval_part = jnp.dot(left, keyval_w[...], preferred_element_type=F32)
    for c in range(n):
        sums_out[c, block : block + kv_per, :] = keyval_part[c * kv_per : (c + 1) * kv_per]
        sums_out[c, block + kv_per : block + kv_per + rows, :] = squares

    for piece in range(QUERY_PIECES):
        query_loads[piece].wait()
        product = jnp.dot(
            scaled_b, query_w[:, piece * step : (piece + 1) * step], preferred_element_type=F32
        )
        for h in range(step // HEAD_DIM):
            head = piece * (step // HEAD_DIM) + h
            low = (head % per) * rows
            sums_out[head // per, low : low + rows, :] = product[
                :, h * HEAD_DIM : (h + 1) * HEAD_DIM
            ]

    pl.semaphore_wait(barrier, n)

    pending = []

    def send(source, target, phase, k):
        copy = pltpu.make_async_remote_copy(
            src_ref=source,
            dst_ref=target,
            send_sem=send_sem.at[phase, k],
            recv_sem=recv_sem.at[phase, k],
            device_id={"seq": lax.rem(me + k, n)},
            device_id_type=MESH,
        )
        copy.start()
        pending.append(copy)
        return copy

    copies = [
        send(sums_out.at[lax.rem(me + k, n)], sums_in.at[k], 0, k) for k in range(1, n)
    ]
    cache_load = pltpu.make_async_copy(cache_hbm, cache, load_sem.at[1 + QUERY_PIECES])
    cache_load.start()
    out_loads = []
    depth = width // OUT_PIECES
    for piece in range(OUT_PIECES):
        part = pl.ds(piece * depth, depth)
        load = pltpu.make_async_copy(
            attend_hbm.at[part], attend_w.at[part], load_sem.at[2 + QUERY_PIECES + piece]
        )
        load.start()
        out_loads.append(load)
    total = sums_out[me]
    for k in range(1, n):
        copies[k - 1].wait_recv()
        total = total + sums_in[k]
    sums_mine[...] = total

    copies = [send(sums_mine, sums_all.at[me], 1, k) for k in range(1, n)]
    sums_all[me] = total

    cols = rows * ctx_dev
    mask_row = lax.broadcasted_iota(jnp.int32, (share * rows, cols), 0) % rows
    mask_col = lax.broadcasted_iota(jnp.int32, (share * rows, cols), 1)
    limit = jnp.zeros((share * rows, cols), jnp.int32)
    for r in range(rows):
        limit = jnp.where(mask_col // ctx_dev == r, lengths_ref[r], limit)
    position = me * ctx_dev + mask_col % ctx_dev
    live = jnp.logical_and(mask_row == mask_col // ctx_dev, position < limit)
    cache_load.wait()

    for copy in copies:
        copy.wait_recv()
    squares_sum = sums_all[0, block + kv_per : block + kv_per + rows, :]
    scale = lax.rsqrt(squares_sum / (feature_dev * n) + EPSILON)
    scale_block = jnp.concatenate([scale] * per, axis=0)
    chunk_heads = share // per
    lane = lax.broadcasted_iota(jnp.int32, (share * rows, HEAD_DIM), 1)
    for head in range(kv_heads):
        query = jnp.concatenate(
            [
                sums_all[c, :block, :] * scale_block
                for c in range(head * chunk_heads, (head + 1) * chunk_heads)
            ],
            axis=0,
        ).astype(BF16)
        lanes = slice(head * HEAD_DIM, (head + 1) * HEAD_DIM)
        keys = cache[0, :, :, lanes].reshape(cols, HEAD_DIM)
        values = cache[1, :, :, lanes].reshape(cols, HEAD_DIM)
        scores = (
            lax.dot_general(
                query, keys, (((1,), (1,)), ((), ())), preferred_element_type=F32
            )
            * score_scale
        )
        scores = jnp.where(live, scores, MASKED)
        block_max = jnp.max(scores, axis=1, keepdims=True)
        weights = jnp.where(live, jnp.exp(scores - block_max), 0.0).astype(BF16)
        block_total = jnp.sum(weights.astype(F32), axis=1, keepdims=True)
        block_out = jnp.dot(weights, values, preferred_element_type=F32)
        stats = jnp.where(lane < HEAD_DIM // 2, block_max, block_total)
        for c in range(chunk_heads):
            part = slice(c * block, (c + 1) * block)
            soft_out[head * chunk_heads + c, :block, :] = block_out[part]
            soft_out[head * chunk_heads + c, block : 2 * block, :] = stats[part]

    copies = [
        send(soft_out.at[lax.rem(me + k, n)], soft_in.at[k], 2, k) for k in range(1, n)
    ]

    keyval = jnp.concatenate(
        [sums_all[c, block : block + kv_per, :] for c in range(n)], axis=0
    )
    keyval = (keyval * jnp.concatenate([scale] * parts, axis=0)).astype(BF16).astype(F32)
    for head in range(kv_heads):
        for kind in range(2):
            low = (2 * head + kind) * rows
            kv_out_ref[:, kind, head * HEAD_DIM : (head + 1) * HEAD_DIM] = keyval[low : low + rows]
    mine = me // chunk_heads
    own_key = keyval[:rows]
    own_value = keyval[rows : 2 * rows]
    for head in range(1, kv_heads):
        here = mine == head
        own_key = jnp.where(here, keyval[2 * head * rows : (2 * head + 1) * rows], own_key)
        own_value = jnp.where(
            here, keyval[(2 * head + 1) * rows : (2 * head + 2) * rows], own_value
        )
    own_key = jnp.concatenate([own_key] * per, axis=0)
    own_value = jnp.concatenate([own_value] * per, axis=0)
    query = (sums_all[me, :block, :] * scale_block).astype(BF16).astype(F32)
    own_score = jnp.sum(query * own_key, axis=1, keepdims=True) * score_scale

    for copy in copies:
        copy.wait_recv()
    chunks = [(soft_out[me, :block, :], soft_out[me, block : 2 * block, :])]
    chunks += [(soft_in[k, :block, :], soft_in[k, block : 2 * block, :]) for k in range(1, n)]
    maxes = [stats[:, :1] for _, stats in chunks]
    totals = [stats[:, HEAD_DIM // 2 : HEAD_DIM // 2 + 1] for _, stats in chunks]
    best = functools.reduce(jnp.maximum, maxes)
    top = jnp.maximum(best, own_score)
    fresh = jnp.exp(own_score - top)
    over = fresh * own_value
    under = fresh
    for (values, _), block_max, block_total in zip(chunks, maxes, totals):
        factor = jnp.exp(block_max - top)
        over = over + factor * values
        under = under + factor * block_total
    attended = (over / under).astype(BF16).astype(F32)
    att_mine[...] = attended

    copies = [send(att_mine, att_all.at[me], 3, k) for k in range(1, n)]
    att_all[me] = attended
    for load in out_loads:
        load.wait()

    def project(source):
        part = att_all[source]
        part = jnp.concatenate([part[j * rows : (j + 1) * rows] for j in range(per)], axis=1)
        first = pl.multiple_of(source * (per * HEAD_DIM), per * HEAD_DIM)
        return jnp.dot(
            part.astype(BF16),
            attend_w[pl.ds(first, per * HEAD_DIM), :],
            preferred_element_type=F32,
        )

    term = project(me)
    for k in range(1, n):
        copies[k - 1].wait_recv()
        term = term + project(lax.rem(me + n - k, n))
    term_mine[...] = term
    swap = pltpu.make_async_remote_copy(
        src_ref=term_mine,
        dst_ref=term_in,
        send_sem=send_sem.at[0, 0],
        recv_sem=recv_sem.at[0, 0],
        device_id={"tp": 1 - core},
        device_id_type=MESH,
    )
    swap.start()
    for copy in pending:
        copy.wait_send()
    swap.wait()
    out_ref[...] = (one_float + (term + term_in[...])).astype(out_ref.dtype)


def fused_device(n, hidden, norm_gain, query_proj, keyval_proj, attend_proj, keyval_cache, lengths):
    rows, feature_dev = hidden.shape
    width = query_proj.shape[1]
    kv_width = keyval_proj.shape[2]
    kv_heads = kv_width // HEAD_DIM
    block = width // HEAD_DIM // n * rows
    kv_rows = 2 * kv_heads * rows
    chunk = -(-(block + kv_rows // n + rows) // 8) * 8
    out_width = attend_proj.shape[1]
    stored = keyval_proj.reshape(feature_dev, 2, kv_heads, HEAD_DIM).transpose(0, 2, 1, 3)
    stored = stored.reshape(feature_dev * 2 * kv_heads, HEAD_DIM)
    vmem = pl.BlockSpec(memory_space=pltpu.VMEM)
    hbm = pl.BlockSpec(memory_space=pl.ANY)
    hidden_out, keyval = pl.pallas_call(
        functools.partial(fused_kernel, n),
        out_shape=(
            pltpu.VMEM((rows, out_width), BF16),
            pltpu.VMEM((rows, 2, kv_width), F32),
        ),
        in_specs=[hbm] * 7,
        out_specs=(vmem, vmem),
        scratch_shapes=[
            pltpu.VMEM(hidden.shape, BF16),
            pltpu.VMEM((1, feature_dev), F32),
            pltpu.SMEM(lengths.shape, jnp.int32),
            pltpu.VMEM(query_proj.shape, BF16),
            pltpu.VMEM(stored.shape, BF16),
            pltpu.VMEM(attend_proj.shape, BF16),
            pltpu.VMEM(keyval_cache.shape, BF16),
            pltpu.VMEM((n, chunk, HEAD_DIM), F32),
            pltpu.VMEM((n, chunk, HEAD_DIM), F32),
            pltpu.VMEM((chunk, HEAD_DIM), F32),
            pltpu.VMEM((n, chunk, HEAD_DIM), F32),
            pltpu.VMEM((n, 2 * block, HEAD_DIM), F32),
            pltpu.VMEM((n, 2 * block, HEAD_DIM), F32),
            pltpu.VMEM((block, HEAD_DIM), F32),
            pltpu.VMEM((n, block, HEAD_DIM), F32),
            pltpu.VMEM((rows, out_width), F32),
            pltpu.VMEM((rows, out_width), F32),
            pltpu.SemaphoreType.DMA((5 + QUERY_PIECES + OUT_PIECES,)),
            pltpu.SemaphoreType.DMA((4, n)),
            pltpu.SemaphoreType.DMA((4, n)),
        ],
        compiler_params=pltpu.CompilerParams(collective_id=0, has_side_effects=True),
    )(
        hidden,
        norm_gain.reshape(1, feature_dev),
        lengths,
        query_proj,
        stored,
        attend_proj,
        keyval_cache,
    )
    return hidden_out, keyval.astype(BF16)


def fits(n, cores, hidden, norm_gain, query_proj, keyval_proj, attend_proj, keyval_cache, lengths):
    rows, feature_dev = hidden.shape
    q_heads = query_proj.shape[1] // HEAD_DIM
    kv_heads = keyval_proj.shape[2] // HEAD_DIM
    if q_heads % n or (2 * kv_heads * rows) % n or cores != 2 or n < 2:
        return False
    per = q_heads // n
    return (
        (q_heads // kv_heads) % per == 0
        and (per * rows) % 8 == 0
        and feature_dev % HEAD_DIM == 0
        and keyval_cache.shape[2] % 16 == 0
        and query_proj.shape[1] % (HEAD_DIM * QUERY_PIECES) == 0
    )


def pick_device(n, cores, *arrays):
    if fits(n, cores, *arrays):
        return fused_device(n, *arrays)
    return on_device(*arrays)


def solution(mesh):
    in_specs = (
        P("grp", "seq"),
        P("seq"),
        P("seq", "tp"),
        P("seq", None, "tp"),
        P("tp", "seq"),
        P(None, "grp", "seq", "tp"),
        P("grp"),
    )
    out_specs = (P("grp", "seq"), P("grp", None, "tp"))
    body = functools.partial(pick_device, mesh.shape["seq"], mesh.shape["tp"])
    return jax.shard_map(
        body, mesh=mesh, in_specs=in_specs, out_specs=out_specs, check_vma=False
    )
```

```python
import functools

import jax
import jax.numpy as jnp
from jax import lax
from jax.experimental import pallas as pl
from jax.experimental.pallas import tpu as pltpu
from jax.sharding import PartitionSpec as P

D = 8192
HEAD_DIM = 128


EPSILON = 1e-05
MASKED = -1e30


def on_device(hidden, norm_gain, query_proj, keyval_proj, attend_proj, keyval_cache, lengths):
    row_count = hidden.shape[0]
    feature_dev = hidden.shape[1]
    seq_rank = lax.axis_index("seq")
    ctx_dev = keyval_cache.shape[2]
    kv_width = keyval_cache.shape[3]
    kv_heads = kv_width // HEAD_DIM
    q_heads = query_proj.shape[1] // HEAD_DIM
    group_share = q_heads // kv_heads
    score_scale = HEAD_DIM ** (-0.5)
    one_float = hidden.astype(jnp.float32)
    scaled = (one_float * norm_gain).astype(jnp.bfloat16)
    squares = jnp.sum(one_float * one_float, axis=1)
    query_part = jnp.dot(scaled, query_proj, preferred_element_type=jnp.float32)
    keyval_part = jnp.dot(
        scaled, keyval_proj.reshape(feature_dev, 2 * kv_width), preferred_element_type=jnp.float32
    ).reshape(row_count, 2, kv_width)
    query_sum, keyval_sum, squares_sum = lax.psum((query_part, keyval_part, squares), "seq")
    scale_two = lax.rsqrt(squares_sum / D + EPSILON)[:, None]
    query = (query_sum * scale_two).astype(jnp.bfloat16)
    new_keyval = (keyval_sum * scale_two[:, :, None]).astype(jnp.bfloat16)
    query_heads = query.reshape(row_count, kv_heads, group_share, HEAD_DIM)
    cache_keys = keyval_cache[0].reshape(row_count, ctx_dev, kv_heads, HEAD_DIM)
    cache_values = keyval_cache[1].reshape(row_count, ctx_dev, kv_heads, HEAD_DIM)
    scores = (
        jnp.einsum("rkgd,rskd->rkgs", query_heads, cache_keys, preferred_element_type=jnp.float32)
        * score_scale
    )
    positions = seq_rank * ctx_dev + jnp.arange(ctx_dev, dtype=jnp.int32)
    live_mask = (positions[None, :] < lengths[:, None])[:, None, None, :]
    scores = jnp.where(live_mask, scores, MASKED)
    block_max = jnp.max(scores, axis=3)
    weights = jnp.where(live_mask, jnp.exp(scores - block_max[..., None]), 0.0).astype(jnp.bfloat16)
    block_total = jnp.sum(lax.optimization_barrier(weights).astype(jnp.float32), axis=3)
    block_out = jnp.einsum(
        "rkgs,rskd->rkgd", weights, cache_values, preferred_element_type=jnp.float32
    )
    best_score = lax.pmax(block_max, "seq")
    factor = jnp.exp(block_max - best_score)
    total_weight, gathered = lax.psum((block_total * factor, block_out * factor[..., None]), "seq")
    own_key = new_keyval[:, 0].reshape(row_count, kv_heads, HEAD_DIM)
    own_value = new_keyval[:, 1].reshape(row_count, kv_heads, HEAD_DIM).astype(jnp.float32)
    own_score = (
        jnp.einsum("rkgd,rkd->rkg", query_heads, own_key, preferred_element_type=jnp.float32)
        * score_scale
    )
    top_score = jnp.maximum(best_score, own_score)
    old_weight = jnp.exp(best_score - top_score)
    fresh_weight = jnp.exp(own_score - top_score)
    attended = (
        old_weight[..., None] * gathered + fresh_weight[..., None] * own_value[:, :, None, :]
    ) / (old_weight * total_weight + fresh_weight)[..., None]
    attended = attended.reshape(row_count, q_heads * HEAD_DIM).astype(jnp.bfloat16)
    attend_term = jnp.dot(attended, attend_proj, preferred_element_type=jnp.float32)
    hidden_out = (one_float + lax.psum(attend_term, "tp")).astype(jnp.bfloat16)
    return (hidden_out, new_keyval)


MESH = pl.DeviceIdType.MESH
F32 = jnp.float32
BF16 = jnp.bfloat16
QUERY_PIECES = 4
OUT_PIECES = 4


def fused_kernel(
    n,
    hidden_hbm,
    gain_hbm,
    lengths_hbm,
    query_hbm,
    keyval_hbm,
    attend_hbm,
    cache_hbm,
    out_ref,
    kv_out_ref,
    hidden_ref,
    gain_ref,
    lengths_ref,
    query_w,
    keyval_w,
    attend_w,
    cache,
    sums_out,
    sums_in,
    sums_mine,
    sums_all,
    soft_out,
    soft_in,
    att_mine,
    att_all,
    term_mine,
    term_in,
    load_sem,
    send_sem,
    recv_sem,
):
    me = lax.axis_index("seq")
    core = lax.axis_index("tp")
    rows, feature_dev = hidden_ref.shape
    width = query_w.shape[1]
    q_heads = width // HEAD_DIM
    ctx_dev = cache.shape[2]
    kv_heads = cache.shape[3] // HEAD_DIM
    share = q_heads // kv_heads
    per = q_heads // n
    block = per * rows
    kv_rows = 2 * kv_heads * rows
    kv_per = kv_rows // n
    score_scale = HEAD_DIM ** (-0.5)

    step = width // QUERY_PIECES
    barrier = pltpu.get_barrier_semaphore()
    for k in range(1, n):
        pl.semaphore_signal(
            barrier, inc=1, device_id={"seq": lax.rem(me + k, n)}, device_id_type=MESH
        )
    pl.semaphore_signal(barrier, inc=1, device_id={"tp": 1 - core}, device_id_type=MESH)

    small_loads = [
        pltpu.make_async_copy(source, target, load_sem.at[2 + QUERY_PIECES + OUT_PIECES + i])
        for i, (source, target) in enumerate(
            [(hidden_hbm, hidden_ref), (gain_hbm, gain_ref), (lengths_hbm, lengths_ref)]
        )
    ]
    for load in small_loads:
        load.start()
    kv_load = pltpu.make_async_copy(keyval_hbm, keyval_w, load_sem.at[0])
    kv_load.start()
    query_loads = []
    for piece in range(QUERY_PIECES):
        cols = pl.ds(piece * step, step)
        load = pltpu.make_async_copy(
            query_hbm.at[:, cols], query_w.at[:, cols], load_sem.at[1 + piece]
        )
        load.start()
        query_loads.append(load)
    for load in small_loads:
        load.wait()
    one_float = hidden_ref[...].astype(F32)
    scaled = one_float * gain_ref[...]
    scaled_b = scaled.astype(BF16)
    squares = jnp.sum(one_float * one_float, axis=1, keepdims=True)
    squares = jnp.broadcast_to(squares, (rows, HEAD_DIM))

    parts = 2 * kv_heads
    groups = feature_dev // HEAD_DIM
    span = HEAD_DIM * parts
    stacked = jnp.concatenate(
        [scaled[:, g * HEAD_DIM : (g + 1) * HEAD_DIM] for g in range(groups)], axis=0
    ).astype(BF16)
    spread_row = lax.broadcasted_iota(jnp.int32, (HEAD_DIM, span), 0)
    spread_col = lax.broadcasted_iota(jnp.int32, (HEAD_DIM, span), 1)
    spread = jnp.where(spread_col // parts == spread_row, 1.0, 0.0).astype(BF16)
    wide = jnp.dot(stacked, spread, preferred_element_type=F32)
    pick_row = lax.broadcasted_iota(jnp.int32, (kv_rows, span), 0) // rows
    pick_col = lax.broadcasted_iota(jnp.int32, (kv_rows, span), 1) % parts
    pick = pick_row == pick_col
    left = jnp.concatenate(
        [
            jnp.where(
                pick, jnp.concatenate([wide[g * rows : (g + 1) * rows]] * parts, axis=0), 0.0
            ).astype(BF16)
            for g in range(groups)
        ],
        axis=1,
    )
    kv_load.wait()
    keyval_part = jnp.dot(left, keyval_w[...], preferred_element_type=F32)
    for c in range(n):
        sums_out[c, block : block + kv_per, :] = keyval_part[c * kv_per : (c + 1) * kv_per]
        sums_out[c, block + kv_per : block + kv_per + rows, :] = squares

    for piece in range(QUERY_PIECES):
        query_loads[piece].wait()
        product = jnp.dot(
            scaled_b, query_w[:, piece * step : (piece + 1) * step], preferred_element_type=F32
        )
        for h in range(step // HEAD_DIM):
            head = piece * (step // HEAD_DIM) + h
            low = (head % per) * rows
            sums_out[head // per, low : low + rows, :] = product[
                :, h * HEAD_DIM : (h + 1) * HEAD_DIM
            ]

    pl.semaphore_wait(barrier, n)

    pending = []

    upper = (2 * me) // n
    peers = []
    for j in range(n - 1):
        down = n - 1 - j - (me + j + 1) // n
        up = j + (n + j - me) // n
        peers.append(down + (up - down) * upper)

    def send(source, target, phase, j):
        copy = pltpu.make_async_remote_copy(
            src_ref=source,
            dst_ref=target,
            send_sem=send_sem.at[phase, j],
            recv_sem=recv_sem.at[phase, me],
            device_id={"seq": peers[j]},
            device_id_type=MESH,
        )
        copy.start()
        pending.append(copy)

    def receive(slots, phase, j):
        pltpu.make_async_remote_copy(
            src_ref=slots.at[peers[j]],
            dst_ref=slots.at[peers[j]],
            send_sem=send_sem.at[phase, j],
            recv_sem=recv_sem.at[phase, peers[j]],
            device_id={"seq": peers[j]},
            device_id_type=MESH,
        ).wait_recv()

    near_first = list(range(n - 2, -1, -1))

    for j in range(n - 1):
        send(sums_out.at[peers[j]], sums_in.at[me], 0, j)
    cache_load = pltpu.make_async_copy(cache_hbm, cache, load_sem.at[1 + QUERY_PIECES])
    cache_load.start()
    out_loads = []
    depth = width // OUT_PIECES
    for piece in range(OUT_PIECES):
        part = pl.ds(piece * depth, depth)
        load = pltpu.make_async_copy(
            attend_hbm.at[part], attend_w.at[part], load_sem.at[2 + QUERY_PIECES + piece]
        )
        load.start()
        out_loads.append(load)
    total = sums_out[me]
    for j in near_first:
        receive(sums_in, 0, j)
        total = total + sums_in[peers[j]]
    sums_mine[...] = total

    for j in range(n - 1):
        send(sums_mine, sums_all.at[me], 1, j)
    sums_all[me] = total

    cols = rows * ctx_dev
    mask_row = lax.broadcasted_iota(jnp.int32, (share * rows, cols), 0) % rows
    mask_col = lax.broadcasted_iota(jnp.int32, (share * rows, cols), 1)
    limit = jnp.zeros((share * rows, cols), jnp.int32)
    for r in range(rows):
        limit = jnp.where(mask_col // ctx_dev == r, lengths_ref[r], limit)
    position = me * ctx_dev + mask_col % ctx_dev
    live = jnp.logical_and(mask_row == mask_col // ctx_dev, position < limit)
    cache_load.wait()

    for j in near_first:
        receive(sums_all, 1, j)
    squares_sum = sums_all[0, block + kv_per : block + kv_per + rows, :]
    scale = lax.rsqrt(squares_sum / (feature_dev * n) + EPSILON)
    scale_block = jnp.concatenate([scale] * per, axis=0)
    chunk_heads = share // per
    lane = lax.broadcasted_iota(jnp.int32, (share * rows, HEAD_DIM), 1)
    for head in range(kv_heads):
        query = jnp.concatenate(
            [
                sums_all[c, :block, :] * scale_block
                for c in range(head * chunk_heads, (head + 1) * chunk_heads)
            ],
            axis=0,
        ).astype(BF16)
        lanes = slice(head * HEAD_DIM, (head + 1) * HEAD_DIM)
        keys = cache[0, :, :, lanes].reshape(cols, HEAD_DIM)
        values = cache[1, :, :, lanes].reshape(cols, HEAD_DIM)
        scores = (
            lax.dot_general(
                query, keys, (((1,), (1,)), ((), ())), preferred_element_type=F32
            )
            * score_scale
        )
        scores = jnp.where(live, scores, MASKED)
        block_max = jnp.max(scores, axis=1, keepdims=True)
        weights = jnp.where(live, jnp.exp(scores - block_max), 0.0).astype(BF16)
        block_total = jnp.sum(weights.astype(F32), axis=1, keepdims=True)
        block_out = jnp.dot(weights, values, preferred_element_type=F32)
        stats = jnp.where(lane < HEAD_DIM // 2, block_max, block_total)
        for c in range(chunk_heads):
            part = slice(c * block, (c + 1) * block)
            soft_out[head * chunk_heads + c, :block, :] = block_out[part]
            soft_out[head * chunk_heads + c, block : 2 * block, :] = stats[part]

    for j in range(n - 1):
        send(soft_out.at[peers[j]], soft_in.at[me], 2, j)

    keyval = jnp.concatenate(
        [sums_all[c, block : block + kv_per, :] for c in range(n)], axis=0
    )
    keyval = (keyval * jnp.concatenate([scale] * parts, axis=0)).astype(BF16).astype(F32)
    for head in range(kv_heads):
        for kind in range(2):
            low = (2 * head + kind) * rows
            kv_out_ref[:, kind, head * HEAD_DIM : (head + 1) * HEAD_DIM] = keyval[low : low + rows]
    mine = me // chunk_heads
    own_key = keyval[:rows]
    own_value = keyval[rows : 2 * rows]
    for head in range(1, kv_heads):
        here = mine == head
        own_key = jnp.where(here, keyval[2 * head * rows : (2 * head + 1) * rows], own_key)
        own_value = jnp.where(
            here, keyval[(2 * head + 1) * rows : (2 * head + 2) * rows], own_value
        )
    own_key = jnp.concatenate([own_key] * per, axis=0)
    own_value = jnp.concatenate([own_value] * per, axis=0)
    query = (sums_all[me, :block, :] * scale_block).astype(BF16).astype(F32)
    own_score = jnp.sum(query * own_key, axis=1, keepdims=True) * score_scale

    for j in near_first:
        receive(soft_in, 2, j)
    chunks = [(soft_out[me, :block, :], soft_out[me, block : 2 * block, :])]
    chunks += [(soft_in[p, :block, :], soft_in[p, block : 2 * block, :]) for p in peers]
    maxes = [stats[:, :1] for _, stats in chunks]
    totals = [stats[:, HEAD_DIM // 2 : HEAD_DIM // 2 + 1] for _, stats in chunks]
    best = functools.reduce(jnp.maximum, maxes)
    top = jnp.maximum(best, own_score)
    fresh = jnp.exp(own_score - top)
    over = fresh * own_value
    under = fresh
    for (values, _), block_max, block_total in zip(chunks, maxes, totals):
        factor = jnp.exp(block_max - top)
        over = over + factor * values
        under = under + factor * block_total
    attended = (over / under).astype(BF16).astype(F32)
    att_mine[...] = attended

    for j in range(n - 1):
        send(att_mine, att_all.at[me], 3, j)
    att_all[me] = attended
    for load in out_loads:
        load.wait()

    def project(source):
        part = att_all[source]
        part = jnp.concatenate([part[j * rows : (j + 1) * rows] for j in range(per)], axis=1)
        first = pl.multiple_of(source * (per * HEAD_DIM), per * HEAD_DIM)
        return jnp.dot(
            part.astype(BF16),
            attend_w[pl.ds(first, per * HEAD_DIM), :],
            preferred_element_type=F32,
        )

    term = project(me)
    for j in near_first:
        receive(att_all, 3, j)
        term = term + project(peers[j])
    term_mine[...] = term
    swap = pltpu.make_async_remote_copy(
        src_ref=term_mine,
        dst_ref=term_in,
        send_sem=send_sem.at[4, 0],
        recv_sem=recv_sem.at[4, 0],
        device_id={"tp": 1 - core},
        device_id_type=MESH,
    )
    swap.start()
    for copy in pending:
        copy.wait_send()
    swap.wait()
    out_ref[...] = (one_float + (term + term_in[...])).astype(out_ref.dtype)


def fused_device(n, hidden, norm_gain, query_proj, keyval_proj, attend_proj, keyval_cache, lengths):
    rows, feature_dev = hidden.shape
    width = query_proj.shape[1]
    kv_width = keyval_proj.shape[2]
    kv_heads = kv_width // HEAD_DIM
    block = width // HEAD_DIM // n * rows
    kv_rows = 2 * kv_heads * rows
    chunk = -(-(block + kv_rows // n + rows) // 8) * 8
    out_width = attend_proj.shape[1]
    stored = keyval_proj.reshape(feature_dev, 2, kv_heads, HEAD_DIM).transpose(0, 2, 1, 3)
    stored = stored.reshape(feature_dev * 2 * kv_heads, HEAD_DIM)
    vmem = pl.BlockSpec(memory_space=pltpu.VMEM)
    hbm = pl.BlockSpec(memory_space=pl.ANY)
    hidden_out, keyval = pl.pallas_call(
        functools.partial(fused_kernel, n),
        out_shape=(
            pltpu.VMEM((rows, out_width), BF16),
            pltpu.VMEM((rows, 2, kv_width), F32),
        ),
        in_specs=[hbm] * 7,
        out_specs=(vmem, vmem),
        scratch_shapes=[
            pltpu.VMEM(hidden.shape, BF16),
            pltpu.VMEM((1, feature_dev), F32),
            pltpu.SMEM(lengths.shape, jnp.int32),
            pltpu.VMEM(query_proj.shape, BF16),
            pltpu.VMEM(stored.shape, BF16),
            pltpu.VMEM(attend_proj.shape, BF16),
            pltpu.VMEM(keyval_cache.shape, BF16),
            pltpu.VMEM((n, chunk, HEAD_DIM), F32),
            pltpu.VMEM((n, chunk, HEAD_DIM), F32),
            pltpu.VMEM((chunk, HEAD_DIM), F32),
            pltpu.VMEM((n, chunk, HEAD_DIM), F32),
            pltpu.VMEM((n, 2 * block, HEAD_DIM), F32),
            pltpu.VMEM((n, 2 * block, HEAD_DIM), F32),
            pltpu.VMEM((block, HEAD_DIM), F32),
            pltpu.VMEM((n, block, HEAD_DIM), F32),
            pltpu.VMEM((rows, out_width), F32),
            pltpu.VMEM((rows, out_width), F32),
            pltpu.SemaphoreType.DMA((5 + QUERY_PIECES + OUT_PIECES,)),
            pltpu.SemaphoreType.DMA((5, n)),
            pltpu.SemaphoreType.DMA((5, n)),
        ],
        compiler_params=pltpu.CompilerParams(collective_id=0, has_side_effects=True),
    )(
        hidden,
        norm_gain.reshape(1, feature_dev),
        lengths,
        query_proj,
        stored,
        attend_proj,
        keyval_cache,
    )
    return hidden_out, keyval.astype(BF16)


def fits(n, cores, hidden, norm_gain, query_proj, keyval_proj, attend_proj, keyval_cache, lengths):
    rows, feature_dev = hidden.shape
    q_heads = query_proj.shape[1] // HEAD_DIM
    kv_heads = keyval_proj.shape[2] // HEAD_DIM
    if q_heads % n or (2 * kv_heads * rows) % n or cores != 2 or n < 2:
        return False
    per = q_heads // n
    return (
        (q_heads // kv_heads) % per == 0
        and (per * rows) % 8 == 0
        and feature_dev % HEAD_DIM == 0
        and keyval_cache.shape[2] % 16 == 0
        and query_proj.shape[1] % (HEAD_DIM * QUERY_PIECES) == 0
    )


def pick_device(n, cores, *arrays):
    if fits(n, cores, *arrays):
        return fused_device(n, *arrays)
    return on_device(*arrays)


def solution(mesh):
    in_specs = (
        P("grp", "seq"),
        P("seq"),
        P("seq", "tp"),
        P("seq", None, "tp"),
        P("tp", "seq"),
        P(None, "grp", "seq", "tp"),
        P("grp"),
    )
    out_specs = (P("grp", "seq"), P("grp", None, "tp"))
    body = functools.partial(pick_device, mesh.shape["seq"], mesh.shape["tp"])
    return jax.shard_map(
        body, mesh=mesh, in_specs=in_specs, out_specs=out_specs, check_vma=False
    )
```
